512 devices in a mesh: band: 128 (over y, z, core), pair: 4 (over x).
Axes of the slice: x: 4, y: 4, z: 16, core: 2. Of those that a mesh axis runs over, the one named last changes fastest.
Arguments:
- orbitals: bfloat16 [512, 262144], P(('band', 'pair')), may hold values from -64 to 64
- partners: int32 [512, 3], P(('band', 'pair')), may hold values from -1 to 511, as said below
Outputs:
- gradient: float32 [512, 262144], P(None, ('band', 'pair'))
The draws below stay inside these ranges and needn't reach their ends.
Inputs may be any that keep to these rules, and one draw needn't show every extreme that they name: `partners`: slot k of orbital i holds either -1 or i XOR (4 * 2**k); j is listed by i exactly when i is listed by j.
All inputs are finite; a program needn't handle non-finite values.
Results may differ from the reference program's by a relative error of at most 0.0008.
The reference program's roundings to bfloat16 on the way (of `term` and `applied`) count: a program that leaves them out, or rounds other values in their place, can miss the bound.
Values may be sent and summed in bfloat16 or wider, within the bound.
No kernel may reach another device: no remote copies, remote signals or barrier semaphores. Data moves between devices by JAX's collectives and lax.ppermute only.
A program may use at most 64 MiB of HBM per device.

```python
import math
import jax
import jax.numpy as jnp
from jax import lax

NG = 64
PARTNERS = 3
NG3 = 262144
ORBITALS = 512
N_PAIR = 4


def draw_orbitals(key, part):
    count = ORBITALS
    index = jnp.arange(count, dtype=jnp.int32)
    cluster = index // N_PAIR // 8
    clusters = count // (8 * N_PAIR)
    centers = jax.random.uniform(jax.random.fold_in(key, 11), (clusters, 3), jnp.float32, 0.25 * NG, 0.75 * NG)
    jitter = jax.random.uniform(jax.random.fold_in(key, 12), (count, 3), jnp.float32, -NG / 12.0, NG / 12.0)
    where = centers[cluster] + jitter
    width = jnp.full((count, 1), NG / 6.0, jnp.float32)
    rough = jnp.clip(jax.random.normal(jax.random.fold_in(key, 14), (count, NG3), jnp.float32), -4.0, 4.0)
    coord = jnp.arange(NG, dtype=jnp.float32)[None, :]
    along_x = jnp.exp(-(coord - where[:, 0:1]) ** 2 / (2.0 * width * width))
    along_y = jnp.exp(-(coord - where[:, 1:2]) ** 2 / (2.0 * width * width))
    along_z = jnp.exp(-(coord - where[:, 2:3]) ** 2 / (2.0 * width * width))
    envelope = along_x[:, :, None, None] * along_y[:, None, :, None] * along_z[:, None, None, :]
    height = (NG / (math.sqrt(math.pi) * width)) ** 1.5
    return (rough * envelope.reshape(count, NG3) * height).astype(jnp.bfloat16)


def draw_partners(key, part):
    count = ORBITALS
    index = jnp.arange(count, dtype=jnp.int32)
    columns = []
    for slot in range(PARTNERS):
        stride = N_PAIR * 2 ** slot
        lowest = index - index // stride % 2 * stride
        flags = jax.random.randint(jax.random.fold_in(key, 21 + slot), (count,), 0, 2)
        forced = jnp.logical_or(lowest % (count // 2) == 0, lowest >= count - 2 * stride)
        live = jnp.logical_or(flags[lowest] == 1, forced)
        mate = index + stride - 2 * (index // stride % 2) * stride
        columns.append(jnp.where(live, mate, -1))
    return jnp.stack(columns, axis=1).astype(jnp.int32)


def setup_inputs(seed: int = 0) -> dict:
    arg_keys = jax.random.split(jax.random.key(seed), 3)
    orbitals = draw_orbitals(jax.random.fold_in(arg_keys[2], 71), 0)
    partners = draw_partners(jax.random.fold_in(arg_keys[2], 71), 0)
    return {"orbitals": orbitals, "partners": partners}


screening = 0.05

def sine_table(size):
    index = jnp.arange(size, dtype=jnp.int32) + 1
    product = index[:, None] * index[None, :] % (2 * (size + 1))
    angle = math.pi * product.astype(jnp.float32) / (size + 1)
    return jnp.sqrt(jnp.float32(2.0 / (size + 1))) * jnp.sin(angle)

def eigen_sum(size):
    steps = jnp.arange(size, dtype=jnp.float32) + 1.0
    lam = 2.0 - 2.0 * jnp.cos(math.pi * steps / (size + 1))
    total = lam[:, None, None] + lam[None, :, None] + lam[None, None, :] + screening
    return total.reshape(size, size * size)

def sine_transform(field, table, doubled):
    size = table.shape[0]
    highest = lax.Precision.HIGHEST
    field = jnp.dot(table, field, precision=highest)
    field = jnp.dot(field.reshape(-1, 2 * size), doubled, precision=highest)
    field = jnp.einsum('ky,xyz->xkz', table, field.reshape(size, size, size), precision=highest)
    return field.reshape(size, size * size)

def screened_solve(density, table, doubled, denom):
    return sine_transform(sine_transform(density, table, doubled) / denom, table, doubled)

def reference(orbitals, partners):
    table = sine_table(NG)
    doubled = jnp.kron(jnp.eye(2, dtype=jnp.float32), table)
    denom = eigen_sum(NG)

    def apply_one(index):
        own = orbitals[index].reshape(NG, NG * NG).astype(jnp.float32)
        total = jnp.zeros((NG, NG * NG), jnp.float32)
        for slot in range(PARTNERS):
            other_index = partners[index, slot]
            other = orbitals[jnp.maximum(other_index, 0)].reshape(NG, NG * NG).astype(jnp.float32)
            potential = screened_solve(own * other, table, doubled, denom)
            term = lax.optimization_barrier((potential * other).astype(jnp.bfloat16))
            total = total + jnp.where(other_index >= 0, term.astype(jnp.float32), 0.0)
        return total.astype(jnp.bfloat16).reshape(NG3)
    applied = lax.map(apply_one, jnp.arange(ORBITALS, dtype=jnp.int32))
    intersection = lax.dot_general(orbitals, applied, (((1,), (1,)), ((), ())), preferred_element_type=jnp.float32)
    intersection = intersection * (1.0 / NG3)
    removed = lax.dot_general(intersection, orbitals.astype(jnp.float32), (((0,), (0,)), ((), ())), precision=lax.Precision.HIGHEST)
    return applied.astype(jnp.float32) - removed
```

```python
import math

import jax
import jax.numpy as jnp
import numpy as np
from jax import lax
from jax.experimental import pallas as pl
from jax.experimental.pallas import tpu as pltpu
from jax.sharding import Mesh
from jax.sharding import PartitionSpec as P

NG = 64
PARTNERS = 3
NG3 = 262144
LANES = 128
ROWS = NG3 // LANES
BAND = ("band_0", "band_1", "band_2")
BAND_PAIR = ("band_0", "band_1", "band_2", "pair")
PLANE = ("band_0", "band_2", "pair")
LINE = "band_1"
F32, BF16 = jnp.float32, jnp.bfloat16
LIMIT = pltpu.CompilerParams(vmem_limit_bytes=16 * 2**20)


screening = 0.05


def partner(value, axis, distance):
    mask = 2**distance
    pairs = [(source, source ^ mask) for source in range(lax.axis_size(axis))]
    return lax.ppermute(value, axis, pairs)


def two_parts(value):
    high = value.astype(BF16)
    return high, (value - high.astype(F32)).astype(BF16)


def tables():
    steps = np.arange(NG) + 1
    table = np.sqrt(2.0 / (NG + 1)) * np.sin(np.pi * (np.outer(steps, steps) % (2 * NG + 2)) / (NG + 1))
    order = np.concatenate([np.arange(0, NG, 2), np.arange(1, NG, 2)])
    high = table.astype(BF16).astype(np.float64)
    low = table - high
    z_high, z_low = (np.kron(np.eye(2), part) for part in (high, low))
    high_y, low_y = (part[order][:, order] for part in (high, low))
    parts = (
        np.concatenate([z_high, z_high], axis=0),
        z_low,
        np.concatenate([high_y, high_y, low_y], axis=1),
        np.concatenate([high, high, low], axis=1),
    )
    return [jnp.asarray(part.astype(BF16)) for part in parts]


def compact_kernel(raw, out):
    def step(n, carry):
        rows = pl.ds(pl.multiple_of(n * 128, 128), 128)
        out[rows] = raw[rows, 0, :]
        return carry

    lax.fori_loop(0, ROWS // 128, step, 0)


def compact(raw):
    return pl.pallas_call(
        compact_kernel, out_shape=jax.ShapeDtypeStruct((ROWS, LANES), BF16), name="compact",
        compiler_params=LIMIT
    )(raw.reshape(ROWS, 1, LANES))


def inverse_kernel(out):
    def lam(index):
        return 2.0 - 2.0 * jnp.cos(math.pi * (index.astype(F32) + 1.0) / (NG + 1))

    shape = (NG, LANES)
    lane = lax.broadcasted_iota(jnp.int32, shape, 1)
    base = lam(lax.broadcasted_iota(jnp.int32, shape, 0)) + lam(lane % NG) + screening

    def step(pair, carry):
        y = lax.broadcasted_iota(jnp.int32, (8, LANES), 1) // NG + 2 * pair
        out[pair] = 1.0 / (base + jnp.broadcast_to(lam(y)[0:1], shape))
        return carry

    lax.fori_loop(0, NG // 2, step, 0)


def inverse_eigen():
    return pl.pallas_call(
        inverse_kernel, out_shape=jax.ShapeDtypeStruct((NG // 2, NG, LANES), F32), name="inverse",
        compiler_params=LIMIT
    )()


def dot(a, b):
    return jnp.dot(a, b, preferred_element_type=F32)


def side(table, value):
    high, low = two_parts(value)
    return dot(table, jnp.concatenate([high, low, high], axis=0))


def along_z(value, z_main, z_low):
    high, low = two_parts(value)
    return dot(jnp.concatenate([high, low], axis=1), z_main) + dot(high, z_low)


def swap_halves(rows, mask):
    first, second = rows[:32], rows[32:]
    top = jnp.where(mask, first, pltpu.roll(second, NG, 1))
    bottom = jnp.where(mask, pltpu.roll(first, NG, 1), second)
    return jnp.concatenate([top, bottom], axis=0)


def along_y(slabs, y_side, mask):
    moved = side(y_side, jnp.concatenate([swap_halves(s, mask) for s in slabs], axis=1))
    return [swap_halves(moved[:, LANES * n : LANES * (n + 1)], mask) for n in range(len(slabs))]


def pair_slabs(block, pair):
    start = 128 * pair
    return [block[start : start + 64], block[start + 64 : start + 128]]


def forward_part(own, other, z_main, z_low, y_side, field, mask):
    def step(n, carry):
        rows = pl.ds(pl.multiple_of(n * 256, 256), 256)
        density = own[rows].astype(F32) * other[rows].astype(F32)
        moved = along_z(density, z_main[...], z_low[...])
        for pair in range(2):
            for m, slab in enumerate(along_y(pair_slabs(moved, pair), y_side[...], mask)):
                field[pl.ds(n * 8 + 4 * pair + 2 * m, 2)] = slab.reshape(2, 32, LANES)
        return carry

    lax.fori_loop(0, ROWS // 256, step, 0)


def middle_part(x_side, inverse, field):
    def step(n, carry):
        group = pl.ds(pl.multiple_of(n * 8, 8), 8)
        block = jnp.transpose(field[:, group, :], (1, 0, 2))
        outs = []
        for pair in range(4):
            lines = [2 * pair, 2 * pair + 1]
            value = jnp.concatenate([block[m] for m in lines], axis=1)
            scale = jnp.concatenate([inverse[n * 8 + m] for m in lines], axis=1)
            value = side(x_side[...], side(x_side[...], value) * scale)
            outs += [value[:, :LANES], value[:, LANES:]]
        field[:, group, :] = jnp.transpose(jnp.stack(outs, axis=0), (1, 0, 2))
        return carry

    lax.fori_loop(0, 4, step, 0)


def backward_block(n, other, z_main, z_low, y_side, field, mask):
    rows = pl.ds(pl.multiple_of(n * 256, 256), 256)
    block = field[pl.ds(n * 8, 8)].reshape(256, LANES)
    slabs = []
    for pair in range(2):
        slabs += along_y(pair_slabs(block, pair), y_side[...], mask)
    moved = along_z(jnp.concatenate(slabs, axis=0), z_main[...], z_low[...])
    return rows, (moved * other[rows].astype(F32)).astype(BF16)


def solve_kernel(own, other, z_main, z_low, y_side, x_side, inverse, term, field):
    mask = lax.broadcasted_iota(jnp.int32, (32, LANES), 1) < NG
    forward_part(own, other, z_main, z_low, y_side, field, mask)
    middle_part(x_side, inverse, field)

    def step(n, carry):
        rows, value = backward_block(n, other, z_main, z_low, y_side, field, mask)
        term[rows] = value
        return carry

    lax.fori_loop(0, ROWS // 256, step, 0)


def last_kernel(
    partners, own, other, z_main, z_low, y_side, x_side, inverse, first, second, out, field
):
    mask = lax.broadcasted_iota(jnp.int32, (32, LANES), 1) < NG
    forward_part(own, other, z_main, z_low, y_side, field, mask)
    middle_part(x_side, inverse, field)

    def step(n, carry):
        rows, third = backward_block(n, other, z_main, z_low, y_side, field, mask)
        total = jnp.zeros((256, LANES), F32)
        for slot, value in enumerate((first[rows], second[rows], third)):
            total = total + jnp.where(partners[0, slot] >= 0, value.astype(F32), 0.0)
        out[pl.ds(n % 2 * 8, 8), n // 2] = total.astype(BF16).reshape(8, 32, LANES)
        return carry

    lax.fori_loop(0, ROWS // 256, step, 0)


FIELD = pltpu.VMEM((NG, NG // 2, LANES), F32)
VMEM = pl.BlockSpec(memory_space=pltpu.VMEM)
SMEM = pl.BlockSpec(memory_space=pltpu.SMEM)


def solve(own, other, parts, inverse):
    return pl.pallas_call(
        solve_kernel,
        out_shape=jax.ShapeDtypeStruct((ROWS, LANES), BF16),
        scratch_shapes=[FIELD],
        name="solve",
        compiler_params=LIMIT,
    )(own, other, *parts, inverse)


def solve_last(partners, own, other, parts, inverse, first, second):
    return pl.pallas_call(
        last_kernel,
        out_shape=jax.ShapeDtypeStruct((16, 4, 32, LANES), BF16),
        in_specs=[SMEM] + [VMEM] * 9,
        scratch_shapes=[FIELD],
        name="last",
        compiler_params=LIMIT,
    )(partners, own, other, *parts, inverse, first, second)


def turn_kernel(value, out):
    for n in range(8):
        block = jnp.transpose(value[:, 16 * n : 16 * n + 16, :], (1, 0, 2))
        out[4 * n : 4 * n + 4] = block.reshape(4, 64, LANES)


def turned(value):
    return pl.pallas_call(
        turn_kernel, out_shape=jax.ShapeDtypeStruct((32, 64, LANES), BF16), name="turn",
        compiler_params=LIMIT
    )(value)


def exchange(value, axes):
    return lax.all_to_all(value, axes, split_axis=0, concat_axis=0, tiled=True)


def regroup(value):
    return exchange(turned(exchange(value.reshape(16, 128, LANES), LINE)), PLANE)


def quarter(slab, q):
    return slab[:, 16 * q : 16 * q + 16, :].reshape(512, LANES)


def whole(slab):
    return jnp.concatenate([quarter(slab, q) for q in range(4)], axis=1)


def overlap_kernel(phi, applied, out):
    value = lax.dot_general(
        whole(applied), whole(phi), (((1,), (1,)), ((), ())), preferred_element_type=F32
    )
    out[...] = value * (1.0 / NG3)


def overlap(phi, applied):
    return pl.pallas_call(
        overlap_kernel, out_shape=jax.ShapeDtypeStruct((512, 512), F32), name="overlap",
        compiler_params=LIMIT
    )(phi, applied)


def project_kernel(overlaps, phi, applied, out):
    high, low = two_parts(overlaps[...])
    cells = whole(phi)
    value = whole(applied).astype(F32) - (dot(high, cells) + dot(low, cells))
    for y in range(4):
        block = value[128 * y : 128 * y + 128].reshape(8, 16, 512)
        out[128 * y : 128 * y + 128] = jnp.transpose(block, (1, 0, 2)).reshape(128, 512)


def project(overlaps, phi, applied):
    return pl.pallas_call(
        project_kernel, out_shape=jax.ShapeDtypeStruct((512, 512), F32), name="project",
        compiler_params=LIMIT
    )(overlaps, phi, applied)


def total_of(value):
    arrived = exchange(value.reshape(32, 16, 512), PLANE).sum(axis=0)
    owned = exchange(arrived.reshape(16, 4, LANES), LINE).sum(axis=0)
    line = exchange(jnp.broadcast_to(owned, (16, 4, LANES)), LINE).reshape(16, 512)
    return exchange(jnp.broadcast_to(line, (32, 16, 512)), PLANE).reshape(512, 512)


def on_device(orbitals, partners):
    mine = compact(orbitals)
    others = [partner(mine, BAND, slot) for slot in range(PARTNERS)]
    parts = tables()
    inverse = inverse_eigen()
    first = solve(mine, others[0], parts, inverse)
    second = solve(mine, others[1], parts, inverse)
    early, first = lax.optimization_barrier((mine, first))
    phi = regroup(early.reshape(4, 16, 32, LANES).transpose(1, 0, 2, 3))
    applied = regroup(solve_last(partners, mine, others[2], parts, inverse, first, second))
    return project(total_of(overlap(phi, applied)), phi, applied)


def solution(mesh):
    torus = Mesh(
        mesh.devices.reshape(4, 16, 2, mesh.shape["pair"]), ("band_0", "band_1", "band_2", "pair")
    )
    in_specs = (P(BAND_PAIR, None), P(BAND_PAIR, None))
    out_specs = P(None, BAND_PAIR)
    return jax.shard_map(
        on_device, mesh=torus, in_specs=in_specs, out_specs=out_specs, check_vma=False
    )
```

```python
import math

import jax
import jax.numpy as jnp
import numpy as np
from jax import lax
from jax.experimental import pallas as pl
from jax.experimental.pallas import tpu as pltpu
from jax.sharding import Mesh
from jax.sharding import PartitionSpec as P


NG = 64
PARTNERS = 3
NG3 = 262144
LANES = 128
ROWS = NG3 // LANES
BAND = ("band_0", "band_1", "band_2")
BAND_PAIR = ("band_0", "band_1", "band_2", "pair")
ACROSS = ("band_1", "pair")
HELD = ("band_0", "band_2")
F32, BF16 = jnp.float32, jnp.bfloat16
LIMIT = pltpu.CompilerParams(vmem_limit_bytes=16 * 2**20)


screening = 0.05


def partner(value, axis, distance):
    mask = 2**distance
    pairs = [(source, source ^ mask) for source in range(lax.axis_size(axis))]
    return lax.ppermute(value, axis, pairs)


def two_parts(value):
    high = value.astype(BF16)
    return high, (value - high.astype(F32)).astype(BF16)


def tables():
    steps = np.arange(NG) + 1
    table = np.sqrt(2.0 / (NG + 1)) * np.sin(np.pi * (np.outer(steps, steps) % (2 * NG + 2)) / (NG + 1))
    order = np.concatenate([np.arange(0, NG, 2), np.arange(1, NG, 2)])
    high = table.astype(BF16).astype(np.float64)
    low = table - high
    z_high, z_low = (np.kron(np.eye(2), part) for part in (high, low))
    high_y, low_y = (part[order][:, order] for part in (high, low))
    parts = (
        np.concatenate([z_high, z_high], axis=0),
        z_low,
        np.concatenate([high_y, high_y, low_y], axis=1),
        np.concatenate([high, high, low], axis=1),
    )
    return [jnp.asarray(part.astype(BF16)) for part in parts]


def compact_kernel(raw, out):
    def step(n, carry):
        rows = pl.ds(pl.multiple_of(n * 128, 128), 128)
        out[rows] = raw[rows, 0, :]
        return carry

    lax.fori_loop(0, ROWS // 128, step, 0)


def compact(raw):
    return pl.pallas_call(
        compact_kernel, out_shape=jax.ShapeDtypeStruct((ROWS, LANES), BF16), name="compact",
        compiler_params=LIMIT
    )(raw.reshape(ROWS, 1, LANES))


def inverse_kernel(out):
    def lam(index):
        return 2.0 - 2.0 * jnp.cos(math.pi * (index.astype(F32) + 1.0) / (NG + 1))

    shape = (NG, LANES)
    lane = lax.broadcasted_iota(jnp.int32, shape, 1)
    base = lam(lax.broadcasted_iota(jnp.int32, shape, 0)) + lam(lane % NG) + screening

    def step(pair, carry):
        y = lax.broadcasted_iota(jnp.int32, (8, LANES), 1) // NG + 2 * pair
        out[pair] = 1.0 / (base + jnp.broadcast_to(lam(y)[0:1], shape))
        return carry

    lax.fori_loop(0, NG // 2, step, 0)


def inverse_eigen():
    return pl.pallas_call(
        inverse_kernel, out_shape=jax.ShapeDtypeStruct((NG // 2, NG, LANES), F32), name="inverse",
        compiler_params=LIMIT
    )()


def dot(a, b):
    return jnp.dot(a, b, preferred_element_type=F32)


def side(table, value):
    high, low = two_parts(value)
    return dot(table, jnp.concatenate([high, low, high], axis=0))


def along_z(value, z_main, z_low):
    high, low = two_parts(value)
    return dot(jnp.concatenate([high, low], axis=1), z_main) + dot(high, z_low)


def swap_halves(rows, mask):
    first, second = rows[:32], rows[32:]
    top = jnp.where(mask, first, pltpu.roll(second, NG, 1))
    bottom = jnp.where(mask, pltpu.roll(first, NG, 1), second)
    return jnp.concatenate([top, bottom], axis=0)


def along_y(slabs, y_side, mask):
    moved = side(y_side, jnp.concatenate([swap_halves(s, mask) for s in slabs], axis=1))
    return [swap_halves(moved[:, LANES * n : LANES * (n + 1)], mask) for n in range(len(slabs))]


def pair_slabs(block, pair):
    start = 128 * pair
    return [block[start : start + 64], block[start + 64 : start + 128]]


def forward_part(own, other, z_main, z_low, y_side, field, mask):
    def step(n, carry):
        rows = pl.ds(pl.multiple_of(n * 256, 256), 256)
        density = own[rows].astype(F32) * other[rows].astype(F32)
        moved = along_z(density, z_main[...], z_low[...])
        for pair in range(2):
            for m, slab in enumerate(along_y(pair_slabs(moved, pair), y_side[...], mask)):
                field[pl.ds(n * 8 + 4 * pair + 2 * m, 2)] = slab.reshape(2, 32, LANES)
        return carry

    lax.fori_loop(0, ROWS // 256, step, 0)


def middle_part(x_side, inverse, field):
    def step(n, carry):
        group = pl.ds(pl.multiple_of(n * 8, 8), 8)
        block = jnp.transpose(field[:, group, :], (1, 0, 2))
        outs = []
        for pair in range(4):
            lines = [2 * pair, 2 * pair + 1]
            value = jnp.concatenate([block[m] for m in lines], axis=1)
            scale = jnp.concatenate([inverse[n * 8 + m] for m in lines], axis=1)
            value = side(x_side[...], side(x_side[...], value) * scale)
            outs += [value[:, :LANES], value[:, LANES:]]
        field[:, group, :] = jnp.transpose(jnp.stack(outs, axis=0), (1, 0, 2))
        return carry

    lax.fori_loop(0, 4, step, 0)


def backward_block(n, other, z_main, z_low, y_side, field, mask):
    rows = pl.ds(pl.multiple_of(n * 256, 256), 256)
    block = field[pl.ds(n * 8, 8)].reshape(256, LANES)
    slabs = []
    for pair in range(2):
        slabs += along_y(pair_slabs(block, pair), y_side[...], mask)
    moved = along_z(jnp.concatenate(slabs, axis=0), z_main[...], z_low[...])
    return rows, (moved * other[rows].astype(F32)).astype(BF16)


def solve_kernel(own, other, z_main, z_low, y_side, x_side, inverse, term, field):
    mask = lax.broadcasted_iota(jnp.int32, (32, LANES), 1) < NG
    forward_part(own, other, z_main, z_low, y_side, field, mask)
    middle_part(x_side, inverse, field)

    def step(n, carry):
        rows, value = backward_block(n, other, z_main, z_low, y_side, field, mask)
        term[rows] = value
        return carry

    lax.fori_loop(0, ROWS // 256, step, 0)


def woven(first, second):
    mask = lax.broadcasted_iota(jnp.int32, first.shape, 1) < 4
    top = jnp.where(mask, first, pltpu.roll(second, 4, 1))
    bottom = jnp.where(mask, pltpu.roll(first, 4, 1), second)
    return jnp.stack([top, bottom], axis=1).reshape(-1, 8, LANES)


def by_owner(rows):
    tiles = rows.reshape(8, 2, 2, 8, LANES)
    return woven(tiles[:, 0].reshape(16, 8, LANES), tiles[:, 1].reshape(16, 8, LANES))


def place(out, n, rows):
    start = pl.multiple_of(n // 2 * 8, 8)
    out[pl.ds(n % 2 * 32, 32), pl.ds(start, 8), :] = by_owner(rows).astype(BF16)


def spread_kernel(mine, out):
    def step(n, carry):
        place(out, n, mine[pl.ds(pl.multiple_of(n * 256, 256), 256)].astype(F32))
        return carry

    lax.fori_loop(0, ROWS // 256, step, 0)


def spread(mine):
    return pl.pallas_call(
        spread_kernel,
        out_shape=jax.ShapeDtypeStruct((64, 32, LANES), BF16),
        name="spread",
        compiler_params=LIMIT,
    )(mine)


def last_kernel(
    partners, own, other, z_main, z_low, y_side, x_side, inverse, first, second, out, field
):
    mask = lax.broadcasted_iota(jnp.int32, (32, LANES), 1) < NG
    forward_part(own, other, z_main, z_low, y_side, field, mask)
    middle_part(x_side, inverse, field)

    def step(n, carry):
        rows, third = backward_block(n, other, z_main, z_low, y_side, field, mask)
        total = jnp.zeros((256, LANES), F32)
        for slot, value in enumerate((first[rows], second[rows], third)):
            total = total + jnp.where(partners[0, slot] >= 0, value.astype(F32), 0.0)
        place(out, n, total)
        return carry

    lax.fori_loop(0, ROWS // 256, step, 0)


FIELD = pltpu.VMEM((NG, NG // 2, LANES), F32)
VMEM = pl.BlockSpec(memory_space=pltpu.VMEM)
SMEM = pl.BlockSpec(memory_space=pltpu.SMEM)


def solve(own, other, parts, inverse):
    return pl.pallas_call(
        solve_kernel,
        out_shape=jax.ShapeDtypeStruct((ROWS, LANES), BF16),
        scratch_shapes=[FIELD],
        name="solve",
        compiler_params=LIMIT,
    )(own, other, *parts, inverse)


def solve_last(partners, own, other, parts, inverse, first, second):
    return pl.pallas_call(
        last_kernel,
        out_shape=jax.ShapeDtypeStruct((64, 32, LANES), BF16),
        in_specs=[SMEM] + [VMEM] * 9,
        scratch_shapes=[FIELD],
        name="last",
        compiler_params=LIMIT,
    )(partners, own, other, *parts, inverse, first, second)


def turn_to(value, out):
    for n in range(2):
        out[16 * n : 16 * n + 16] = jnp.transpose(value[:, 16 * n : 16 * n + 16, :], (1, 0, 2))


def turned(value):
    return pl.pallas_call(
        turn_to,
        out_shape=jax.ShapeDtypeStruct((32, 64, LANES), BF16),
        name="turn",
        compiler_params=LIMIT,
    )(value)


def exchange(value, axes):
    return lax.all_to_all(value, axes, split_axis=0, concat_axis=0, tiled=True)


def two_rows(slab, n):
    return jnp.concatenate([slab[2 * n], slab[2 * n + 1]], axis=1)


def all_two_rows(slabs, n):
    return jnp.concatenate([two_rows(slab, n) for slab in slabs], axis=0)


def overlap_kernel(applied, *refs):
    phis, (out, slab) = refs[:8], refs[8:]
    turn_to(applied, slab)

    def step(n, total):
        return total + lax.dot_general(
            two_rows(slab, n),
            all_two_rows(phis, n),
            (((1,), (1,)), ((), ())),
            preferred_element_type=F32,
        )

    total = lax.fori_loop(0, 16, step, jnp.zeros((64, 512), F32)) * (1.0 / NG3)
    for n in range(4):
        out[:, n, :] = total[:, LANES * n : LANES * (n + 1)]


def overlap(applied, phis):
    return pl.pallas_call(
        overlap_kernel,
        out_shape=(
            jax.ShapeDtypeStruct((64, 4, LANES), F32),
            jax.ShapeDtypeStruct((32, 64, LANES), BF16),
        ),
        name="overlap",
        compiler_params=LIMIT,
    )(applied, *phis)


def project_kernel(overlaps, slab, *refs):
    phis, out = refs[:8], refs[8]
    high, low = two_parts(jnp.concatenate([overlaps[:, n, :] for n in range(4)], axis=1))

    def step(n, carry):
        cells = all_two_rows(phis, n)
        value = two_rows(slab, n).astype(F32) - (dot(high, cells) + dot(low, cells))
        out[2 * n] = value[:, :LANES]
        out[2 * n + 1] = value[:, LANES:]
        return carry

    lax.fori_loop(0, 16, step, 0)


def project(overlaps, slab, phis):
    return pl.pallas_call(
        project_kernel,
        out_shape=jax.ShapeDtypeStruct((32, 64, LANES), F32),
        name="project",
        compiler_params=LIMIT,
    )(overlaps, slab, *phis)


def settle_kernel(arrived, out):
    for y in range(4):
        for q in range(4):
            both = [arrived[2 * y + core, 64 * q : 64 * q + 64, :].reshape(8, 8, LANES) for core in range(2)]
            out[128 * y : 128 * y + 128, LANES * q : LANES * (q + 1)] = woven(*both).reshape(128, LANES)


def settle(arrived):
    return pl.pallas_call(
        settle_kernel,
        out_shape=jax.ShapeDtypeStruct((512, 512), F32),
        name="settle",
        compiler_params=LIMIT,
    )(arrived)


def shifted(value, axis, distance):
    size = lax.axis_size(axis)
    return lax.ppermute(value, axis, [(n, (n + distance) % size) for n in range(size)])


def gathered(slab):
    slabs = [slab]
    for distance in (1, 3, 2):
        slabs.append(shifted(slab, "band_0", distance))
    return slabs + [shifted(value, "band_2", 1) for value in slabs]


def total_of(value):
    owned = exchange(value, ACROSS).sum(axis=0)
    return exchange(jnp.broadcast_to(owned, value.shape), ACROSS)


def on_device(orbitals, partners):
    mine = compact(orbitals)
    others = []
    for slot in range(PARTNERS):
        others.append(partner(mine, BAND, slot))
    parts = tables()
    inverse = inverse_eigen()
    first = solve(mine, others[0], parts, inverse)
    first, others[1] = lax.optimization_barrier((first, others[1]))
    second = solve(mine, others[1], parts, inverse)
    applied = solve_last(partners, mine, others[2], parts, inverse, first, second)
    phi = exchange(spread(mine), ACROSS)
    phis = gathered(turned(phi))
    applied = exchange(applied, ACROSS)
    partial, slab = overlap(applied, phis)
    gradient = project(total_of(partial), slab, phis)
    return settle(exchange(gradient.reshape(8, 256, LANES), HELD))


def solution(mesh):
    torus = Mesh(
        mesh.devices.reshape(4, 16, 2, mesh.shape["pair"]), ("band_0", "band_1", "band_2", "pair")
    )
    in_specs = (P(BAND_PAIR, None), P(BAND_PAIR, None))
    out_specs = P(None, BAND_PAIR)
    return jax.shard_map(
        on_device, mesh=torus, in_specs=in_specs, out_specs=out_specs, check_vma=False
    )
```

```python
import math

import jax
import jax.numpy as jnp
import numpy as np
from jax import lax
from jax.experimental import pallas as pl
from jax.experimental.pallas import tpu as pltpu
from jax.sharding import Mesh
from jax.sharding import PartitionSpec as P


NG = 64
PARTNERS = 3
NG3 = 262144
LANES = 128
ROWS = NG3 // LANES
BAND = ("y_high", "y_low", "z", "core")
BAND_PAIR = BAND + ("x_high", "x_low")
ACROSS = ("y_high", "x_high", "z")
HELD = ("y_low", "core", "x_low")
F32, BF16 = jnp.float32, jnp.bfloat16
LIMIT = pltpu.CompilerParams(vmem_limit_bytes=16 * 2**20)


screening = 0.05


def partner(value, axis, distance):
    mask = 2**distance
    pairs = [(source, source ^ mask) for source in range(lax.axis_size(axis))]
    return lax.ppermute(value, axis, pairs)


def two_parts(value):
    high = value.astype(BF16)
    return high, (value - high.astype(F32)).astype(BF16)


def tables():
    steps = np.arange(NG) + 1
    table = np.sqrt(2.0 / (NG + 1)) * np.sin(np.pi * (np.outer(steps, steps) % (2 * NG + 2)) / (NG + 1))
    order = np.concatenate([np.arange(0, NG, 2), np.arange(1, NG, 2)])
    high = table.astype(BF16).astype(np.float64)
    low = table - high
    z_high, z_low = (np.kron(np.eye(2), part) for part in (high, low))
    high_y, low_y = (part[order][:, order] for part in (high, low))
    parts = (
        np.concatenate([z_high, z_high], axis=0),
        z_low,
        np.concatenate([high_y, high_y, low_y], axis=1),
        np.concatenate([high, high, low], axis=1),
    )
    return [jnp.asarray(part.astype(BF16)) for part in parts]


def compact_kernel(raw, out):
    def step(n, carry):
        rows = pl.ds(pl.multiple_of(n * 128, 128), 128)
        out[rows] = raw[rows, 0, :]
        return carry

    lax.fori_loop(0, ROWS // 128, step, 0)


def compact(raw):
    return pl.pallas_call(
        compact_kernel, out_shape=jax.ShapeDtypeStruct((ROWS, LANES), BF16), name="compact",
        compiler_params=LIMIT
    )(raw.reshape(ROWS, 1, LANES))


def inverse_kernel(out):
    def lam(index):
        return 2.0 - 2.0 * jnp.cos(math.pi * (index.astype(F32) + 1.0) / (NG + 1))

    shape = (NG, LANES)
    lane = lax.broadcasted_iota(jnp.int32, shape, 1)
    base = lam(lax.broadcasted_iota(jnp.int32, shape, 0)) + lam(lane % NG) + screening

    def step(pair, carry):
        y = lax.broadcasted_iota(jnp.int32, (8, LANES), 1) // NG + 2 * pair
        out[pair] = 1.0 / (base + jnp.broadcast_to(lam(y)[0:1], shape))
        return carry

    lax.fori_loop(0, NG // 2, step, 0)


def inverse_eigen():
    return pl.pallas_call(
        inverse_kernel, out_shape=jax.ShapeDtypeStruct((NG // 2, NG, LANES), F32), name="inverse",
        compiler_params=LIMIT
    )()


def dot(a, b):
    return jnp.dot(a, b, preferred_element_type=F32)


def side(table, value):
    high, low = two_parts(value)
    return dot(table, jnp.concatenate([high, low, high], axis=0))


def along_z(value, z_main, z_low):
    high, low = two_parts(value)
    return dot(jnp.concatenate([high, low], axis=1), z_main) + dot(high, z_low)


def swap_halves(rows, mask):
    first, second = rows[:32], rows[32:]
    top = jnp.where(mask, first, pltpu.roll(second, NG, 1))
    bottom = jnp.where(mask, pltpu.roll(first, NG, 1), second)
    return jnp.concatenate([top, bottom], axis=0)


def along_y(slabs, y_side, mask):
    moved = side(y_side, jnp.concatenate([swap_halves(s, mask) for s in slabs], axis=1))
    return [swap_halves(moved[:, LANES * n : LANES * (n + 1)], mask) for n in range(len(slabs))]


def pair_slabs(block, pair):
    start = 128 * pair
    return [block[start : start + 64], block[start + 64 : start + 128]]


def forward_part(own, other, z_main, z_low, y_side, field, mask):
    def step(n, carry):
        rows = pl.ds(pl.multiple_of(n * 256, 256), 256)
        density = own[rows].astype(F32) * other[rows].astype(F32)
        moved = along_z(density, z_main[...], z_low[...])
        for pair in range(2):
            for m, slab in enumerate(along_y(pair_slabs(moved, pair), y_side[...], mask)):
                field[pl.ds(n * 8 + 4 * pair + 2 * m, 2)] = slab.reshape(2, 32, LANES)
        return carry

    lax.fori_loop(0, ROWS // 256, step, 0, unroll=2)


def middle_part(x_side, inverse, field):
    def step(n, carry):
        group = pl.ds(pl.multiple_of(n * 8, 8), 8)
        block = jnp.transpose(field[:, group, :], (1, 0, 2))
        outs = []
        for pair in range(4):
            lines = [2 * pair, 2 * pair + 1]
            value = jnp.concatenate([block[m] for m in lines], axis=1)
            scale = jnp.concatenate([inverse[n * 8 + m] for m in lines], axis=1)
            value = side(x_side[...], side(x_side[...], value) * scale)
            outs += [value[:, :LANES], value[:, LANES:]]
        field[:, group, :] = jnp.transpose(jnp.stack(outs, axis=0), (1, 0, 2))
        return carry

    lax.fori_loop(0, 4, step, 0, unroll=2)


def backward_block(n, other, z_main, z_low, y_side, field, mask):
    rows = pl.ds(pl.multiple_of(n * 256, 256), 256)
    block = field[pl.ds(n * 8, 8)].reshape(256, LANES)
    slabs = []
    for pair in range(2):
        slabs += along_y(pair_slabs(block, pair), y_side[...], mask)
    moved = along_z(jnp.concatenate(slabs, axis=0), z_main[...], z_low[...])
    return rows, (moved * other[rows].astype(F32)).astype(BF16)


def solve_kernel(own, other, z_main, z_low, y_side, x_side, inverse, term, field):
    mask = lax.broadcasted_iota(jnp.int32, (32, LANES), 1) < NG
    forward_part(own, other, z_main, z_low, y_side, field, mask)
    middle_part(x_side, inverse, field)

    def step(n, carry):
        rows, value = backward_block(n, other, z_main, z_low, y_side, field, mask)
        term[rows] = value
        return carry

    lax.fori_loop(0, ROWS // 256, step, 0, unroll=2)


def place(out, n, rows):
    tiles = rows.astype(BF16).reshape(8, 2, 2, 8, LANES)
    for core in range(2):
        start = pl.multiple_of((n // 2 % 2 * 2 + core) * 8, 8)
        for x_high in range(2):
            owner = (n // 4 * 2 + x_high) * 16 + n % 2 * 8
            out[pl.ds(owner, 8), pl.ds(start, 8), :] = tiles[:, core, x_high]


def spread_kernel(mine, out):
    def step(n, carry):
        place(out, n, mine[pl.ds(pl.multiple_of(n * 256, 256), 256)])
        return carry

    lax.fori_loop(0, ROWS // 256, step, 0, unroll=2)


def spread(mine):
    return pl.pallas_call(
        spread_kernel,
        out_shape=jax.ShapeDtypeStruct((64, 32, LANES), BF16),
        name="spread",
        compiler_params=LIMIT,
    )(mine)


def last_kernel(
    partners, own, other, z_main, z_low, y_side, x_side, inverse, first, second, out, field
):
    mask = lax.broadcasted_iota(jnp.int32, (32, LANES), 1) < NG
    forward_part(own, other, z_main, z_low, y_side, field, mask)
    middle_part(x_side, inverse, field)

    def step(n, carry):
        rows, third = backward_block(n, other, z_main, z_low, y_side, field, mask)
        total = jnp.zeros((256, LANES), F32)
        for slot, value in enumerate((first[rows], second[rows], third)):
            total = total + jnp.where(partners[0, slot] >= 0, value.astype(F32), 0.0)
        place(out, n, total)
        return carry

    lax.fori_loop(0, ROWS // 256, step, 0, unroll=2)


FIELD = pltpu.VMEM((NG, NG // 2, LANES), F32)
VMEM = pl.BlockSpec(memory_space=pltpu.VMEM)
SMEM = pl.BlockSpec(memory_space=pltpu.SMEM)


def solve(own, other, parts, inverse):
    return pl.pallas_call(
        solve_kernel,
        out_shape=jax.ShapeDtypeStruct((ROWS, LANES), BF16),
        scratch_shapes=[FIELD],
        name="solve",
        compiler_params=LIMIT,
    )(own, other, *parts, inverse)


def solve_last(partners, own, other, parts, inverse, first, second):
    return pl.pallas_call(
        last_kernel,
        out_shape=jax.ShapeDtypeStruct((64, 32, LANES), BF16),
        in_specs=[SMEM] + [VMEM] * 9,
        scratch_shapes=[FIELD],
        name="last",
        compiler_params=LIMIT,
    )(partners, own, other, *parts, inverse, first, second)


def turn_to(value, out):
    for n in range(2):
        out[16 * n : 16 * n + 16] = jnp.transpose(value[:, 16 * n : 16 * n + 16, :], (1, 0, 2))


def turned(value):
    return pl.pallas_call(
        turn_to,
        out_shape=jax.ShapeDtypeStruct((32, 64, LANES), BF16),
        name="turn",
        compiler_params=LIMIT,
    )(value)


def exchange(value, axes):
    return lax.all_to_all(value, axes, split_axis=0, concat_axis=0, tiled=True)


def two_rows(slab, n):
    return jnp.concatenate([slab[2 * n], slab[2 * n + 1]], axis=1)


def all_two_rows(slabs, n):
    return jnp.concatenate([two_rows(slab, n) for slab in slabs], axis=0)


def overlap_kernel(applied, *refs):
    phis, (out, slab) = refs[:8], refs[8:]
    turn_to(applied, slab)

    def step(n, total):
        return total + lax.dot_general(
            two_rows(slab, n),
            all_two_rows(phis, n),
            (((1,), (1,)), ((), ())),
            preferred_element_type=F32,
        )

    total = lax.fori_loop(0, 16, step, jnp.zeros((64, 512), F32), unroll=4) * (1.0 / NG3)
    for n in range(4):
        out[:, n, :] = total[:, LANES * n : LANES * (n + 1)]


def overlap(applied, phis):
    return pl.pallas_call(
        overlap_kernel,
        out_shape=(
            jax.ShapeDtypeStruct((64, 4, LANES), F32),
            jax.ShapeDtypeStruct((32, 64, LANES), BF16),
        ),
        name="overlap",
        compiler_params=LIMIT,
    )(applied, *phis)


def project_kernel(overlaps, slab, *refs):
    phis, out = refs[:8], refs[8]
    parts = jnp.concatenate(
        two_parts(jnp.concatenate([overlaps[:, n, :] for n in range(4)], axis=1)), axis=0
    )

    def step(n, carry):
        both = dot(parts, all_two_rows(phis, n))
        value = two_rows(slab, n).astype(F32) - (both[:64] + both[64:])
        out[2 * n] = value[:, :LANES]
        out[2 * n + 1] = value[:, LANES:]
        return carry

    lax.fori_loop(0, 16, step, 0, unroll=4)


def project(overlaps, slab, phis):
    return pl.pallas_call(
        project_kernel,
        out_shape=jax.ShapeDtypeStruct((32, 64, LANES), F32),
        name="project",
        compiler_params=LIMIT,
    )(overlaps, slab, *phis)


def settle_kernel(arrived, out):
    for y in range(4):
        for q in range(4):
            lines = []
            for core in range(2):
                for x in range(4):
                    start = 64 * q + 32 * (y // 2) + 16 * (x // 2)
                    lines.append(arrived[4 * (y % 2) + 2 * core + x % 2, start : start + 16, :])
            rows = jnp.transpose(jnp.stack(lines, axis=0), (1, 0, 2)).reshape(128, LANES)
            out[128 * y : 128 * y + 128, LANES * q : LANES * (q + 1)] = rows


def settle(arrived):
    return pl.pallas_call(
        settle_kernel,
        out_shape=jax.ShapeDtypeStruct((512, 512), F32),
        name="settle",
        compiler_params=LIMIT,
    )(arrived)


def flipped(value, axes, mask):
    size = lax.axis_size(axes)
    return lax.ppermute(value, axes, [(n, n ^ mask) for n in range(size)])


def gathered(slab):
    slabs = [slab]
    for mask in (1, 2, 3):
        slabs.append(flipped(slab, ("y_low", "x_low"), mask))
    return slabs + [flipped(value, "core", 1) for value in slabs]


def total_of(value):
    owned = exchange(value, ACROSS).sum(axis=0)
    return exchange(jnp.broadcast_to(owned, value.shape), ACROSS)


def on_device(orbitals, partners):
    mine = compact(orbitals)
    others = []
    for slot in range(PARTNERS):
        others.append(partner(mine, BAND, slot))
    parts = tables()
    inverse = inverse_eigen()
    first = solve(mine, others[0], parts, inverse)
    first, others[1] = lax.optimization_barrier((first, others[1]))
    second = solve(mine, others[1], parts, inverse)
    applied = solve_last(partners, mine, others[2], parts, inverse, first, second)
    phi = exchange(spread(mine), ACROSS)
    phis = gathered(turned(phi))
    applied = exchange(applied, ACROSS)
    partial, slab = overlap(applied, phis)
    gradient = project(total_of(partial), slab, phis)
    return settle(exchange(gradient.reshape(8, 256, LANES), HELD))


def solution(mesh):
    torus = Mesh(mesh.devices.reshape(2, 2, 16, 2, 2, 2), BAND_PAIR)
    in_specs = (P(BAND_PAIR, None), P(BAND_PAIR, None))
    out_specs = P(None, BAND_PAIR)
    return jax.shard_map(
        on_device, mesh=torus, in_specs=in_specs, out_specs=out_specs, check_vma=False
    )
```

```python
import math

import jax
import jax.numpy as jnp
import numpy as np
from jax import lax
from jax.experimental import pallas as pl
from jax.experimental.pallas import tpu as pltpu
from jax.sharding import Mesh
from jax.sharding import PartitionSpec as P


NG = 64
PARTNERS = 3
NG3 = 262144
LANES = 128
ROWS = NG3 // LANES
BAND = ("band_0", "band_1", "band_2")
BAND_PAIR = ("band_0", "band_1", "band_2", "pair")
ACROSS = ("band_1", "pair")
HELD = ("band_0", "band_2")
F32, BF16 = jnp.float32, jnp.bfloat16
LIMIT = pltpu.CompilerParams(vmem_limit_bytes=16 * 2**20)


screening = 0.05


def partner(value, axis, distance):
    mask = 2**distance
    pairs = [(source, source ^ mask) for source in range(lax.axis_size(axis))]
    return lax.ppermute(value, axis, pairs)


def two_parts(value):
    high = value.astype(BF16)
    return high, (value - high.astype(F32)).astype(BF16)


def tables():
    steps = np.arange(NG) + 1
    table = np.sqrt(2.0 / (NG + 1)) * np.sin(np.pi * (np.outer(steps, steps) % (2 * NG + 2)) / (NG + 1))
    order = np.concatenate([np.arange(0, NG, 2), np.arange(1, NG, 2)])
    high = table.astype(BF16).astype(np.float64)
    low = table - high
    z_high, z_low = (np.kron(np.eye(2), part) for part in (high, low))
    high_y, low_y = (part[order][:, order] for part in (high, low))
    parts = (
        np.concatenate([z_high, z_high], axis=0),
        z_low,
        np.concatenate([high_y, high_y, low_y], axis=1),
        np.concatenate([high, high, low], axis=1),
    )
    return [jnp.asarray(part.astype(BF16)) for part in parts]


def compact_kernel(raw, out):
    def step(n, carry):
        rows = pl.ds(pl.multiple_of(n * 128, 128), 128)
        out[rows] = raw[rows, 0, :]
        return carry

    lax.fori_loop(0, ROWS // 128, step, 0)


def compact(raw):
    return pl.pallas_call(
        compact_kernel, out_shape=jax.ShapeDtypeStruct((ROWS, LANES), BF16), name="compact",
        compiler_params=LIMIT
    )(raw.reshape(ROWS, 1, LANES))


def inverse_kernel(out):
    def lam(index):
        return 2.0 - 2.0 * jnp.cos(math.pi * (index.astype(F32) + 1.0) / (NG + 1))

    shape = (NG, LANES)
    lane = lax.broadcasted_iota(jnp.int32, shape, 1)
    base = lam(lax.broadcasted_iota(jnp.int32, shape, 0)) + lam(lane % NG) + screening

    def step(pair, carry):
        y = lax.broadcasted_iota(jnp.int32, (8, LANES), 1) // NG + 2 * pair
        out[pair] = 1.0 / (base + jnp.broadcast_to(lam(y)[0:1], shape))
        return carry

    lax.fori_loop(0, NG // 2, step, 0)


def inverse_eigen():
    return pl.pallas_call(
        inverse_kernel, out_shape=jax.ShapeDtypeStruct((NG // 2, NG, LANES), F32), name="inverse",
        compiler_params=LIMIT
    )()


def dot(a, b):
    return jnp.dot(a, b, preferred_element_type=F32)


def side(table, value):
    high, low = two_parts(value)
    return dot(table, jnp.concatenate([high, low, high], axis=0))


def along_z(value, z_main, z_low):
    high, low = two_parts(value)
    return dot(jnp.concatenate([high, low], axis=1), z_main) + dot(high, z_low)


def swap_halves(rows, mask):
    first, second = rows[:32], rows[32:]
    top = jnp.where(mask, first, pltpu.roll(second, NG, 1))
    bottom = jnp.where(mask, pltpu.roll(first, NG, 1), second)
    return jnp.concatenate([top, bottom], axis=0)


def along_y(slabs, y_side, mask):
    moved = side(y_side, jnp.concatenate([swap_halves(s, mask) for s in slabs], axis=1))
    return [swap_halves(moved[:, LANES * n : LANES * (n + 1)], mask) for n in range(len(slabs))]


def pair_slabs(block, pair):
    start = 128 * pair
    return [block[start : start + 64], block[start + 64 : start + 128]]


def forward_part(own, other, z_main, z_low, y_side, field, mask):
    def step(n, carry):
        rows = pl.ds(pl.multiple_of(n * 256, 256), 256)
        density = own[rows].astype(F32) * other[rows].astype(F32)
        moved = along_z(density, z_main[...], z_low[...])
        for pair in range(2):
            for m, slab in enumerate(along_y(pair_slabs(moved, pair), y_side[...], mask)):
                field[pl.ds(n * 8 + 4 * pair + 2 * m, 2)] = slab.reshape(2, 32, LANES)
        return carry

    lax.fori_loop(0, ROWS // 256, step, 0, unroll=2)


def middle_part(x_side, inverse, field):
    def step(n, carry):
        group = pl.ds(pl.multiple_of(n * 8, 8), 8)
        block = jnp.transpose(field[:, group, :], (1, 0, 2))
        outs = []
        for pair in range(4):
            lines = [2 * pair, 2 * pair + 1]
            value = jnp.concatenate([block[m] for m in lines], axis=1)
            scale = jnp.concatenate([inverse[n * 8 + m] for m in lines], axis=1)
            value = side(x_side[...], side(x_side[...], value) * scale)
            outs += [value[:, :LANES], value[:, LANES:]]
        field[:, group, :] = jnp.transpose(jnp.stack(outs, axis=0), (1, 0, 2))
        return carry

    lax.fori_loop(0, 4, step, 0, unroll=2)


def backward_block(n, other, z_main, z_low, y_side, field, mask):
    rows = pl.ds(pl.multiple_of(n * 256, 256), 256)
    block = field[pl.ds(n * 8, 8)].reshape(256, LANES)
    slabs = []
    for pair in range(2):
        slabs += along_y(pair_slabs(block, pair), y_side[...], mask)
    moved = along_z(jnp.concatenate(slabs, axis=0), z_main[...], z_low[...])
    return rows, (moved * other[rows].astype(F32)).astype(BF16)


def solve_kernel(own, other, z_main, z_low, y_side, x_side, inverse, term, field):
    mask = lax.broadcasted_iota(jnp.int32, (32, LANES), 1) < NG
    forward_part(own, other, z_main, z_low, y_side, field, mask)
    middle_part(x_side, inverse, field)

    def step(n, carry):
        rows, value = backward_block(n, other, z_main, z_low, y_side, field, mask)
        term[rows] = value
        return carry

    lax.fori_loop(0, ROWS // 256, step, 0, unroll=2)


def woven(first, second):
    mask = lax.broadcasted_iota(jnp.int32, first.shape, 1) < 4
    top = jnp.where(mask, first, pltpu.roll(second, 4, 1))
    bottom = jnp.where(mask, pltpu.roll(first, 4, 1), second)
    return jnp.stack([top, bottom], axis=1).reshape(-1, 8, LANES)


def by_owner(rows):
    tiles = rows.reshape(8, 2, 2, 8, LANES)
    return woven(tiles[:, 0].reshape(16, 8, LANES), tiles[:, 1].reshape(16, 8, LANES))


def place(out, n, rows):
    start = pl.multiple_of(n // 2 * 8, 8)
    out[pl.ds(n % 2 * 32, 32), pl.ds(start, 8), :] = by_owner(rows).astype(BF16)


def spread_kernel(mine, out):
    def step(n, carry):
        place(out, n, mine[pl.ds(pl.multiple_of(n * 256, 256), 256)].astype(F32))
        return carry

    lax.fori_loop(0, ROWS // 256, step, 0, unroll=2)


def spread(mine):
    return pl.pallas_call(
        spread_kernel,
        out_shape=jax.ShapeDtypeStruct((64, 32, LANES), BF16),
        name="spread",
        compiler_params=LIMIT,
    )(mine)


def last_kernel(
    partners, own, other, z_main, z_low, y_side, x_side, inverse, first, second, out, field
):
    mask = lax.broadcasted_iota(jnp.int32, (32, LANES), 1) < NG
    forward_part(own, other, z_main, z_low, y_side, field, mask)
    middle_part(x_side, inverse, field)

    def step(n, carry):
        rows, third = backward_block(n, other, z_main, z_low, y_side, field, mask)
        total = jnp.zeros((256, LANES), F32)
        for slot, value in enumerate((first[rows], second[rows], third)):
            total = total + jnp.where(partners[0, slot] >= 0, value.astype(F32), 0.0)
        place(out, n, total)
        return carry

    lax.fori_loop(0, ROWS // 256, step, 0, unroll=2)


FIELD = pltpu.VMEM((NG, NG // 2, LANES), F32)
VMEM = pl.BlockSpec(memory_space=pltpu.VMEM)
SMEM = pl.BlockSpec(memory_space=pltpu.SMEM)


def solve(own, other, parts, inverse):
    return pl.pallas_call(
        solve_kernel,
        out_shape=jax.ShapeDtypeStruct((ROWS, LANES), BF16),
        scratch_shapes=[FIELD],
        name="solve",
        compiler_params=LIMIT,
    )(own, other, *parts, inverse)


def solve_last(partners, own, other, parts, inverse, first, second):
    return pl.pallas_call(
        last_kernel,
        out_shape=jax.ShapeDtypeStruct((64, 32, LANES), BF16),
        in_specs=[SMEM] + [VMEM] * 9,
        scratch_shapes=[FIELD],
        name="last",
        compiler_params=LIMIT,
    )(partners, own, other, *parts, inverse, first, second)


def turn_to(value, out):
    for n in range(2):
        out[16 * n : 16 * n + 16] = jnp.transpose(value[:, 16 * n : 16 * n + 16, :], (1, 0, 2))


def turned(value):
    return pl.pallas_call(
        turn_to,
        out_shape=jax.ShapeDtypeStruct((32, 64, LANES), BF16),
        name="turn",
        compiler_params=LIMIT,
    )(value)


def exchange(value, axes):
    return lax.all_to_all(value, axes, split_axis=0, concat_axis=0, tiled=True)


def two_rows(slab, n):
    return jnp.concatenate([slab[2 * n], slab[2 * n + 1]], axis=1)


def all_two_rows(slabs, n):
    return jnp.concatenate([two_rows(slab, n) for slab in slabs], axis=0)


def overlap_kernel(applied, *refs):
    phis, (out, slab) = refs[:8], refs[8:]
    turn_to(applied, slab)

    def step(n, total):
        return total + lax.dot_general(
            two_rows(slab, n),
            all_two_rows(phis, n),
            (((1,), (1,)), ((), ())),
            preferred_element_type=F32,
        )

    total = lax.fori_loop(0, 16, step, jnp.zeros((64, 512), F32), unroll=4) * (1.0 / NG3)
    for n in range(4):
        out[:, n, :] = total[:, LANES * n : LANES * (n + 1)]


def overlap(applied, phis):
    return pl.pallas_call(
        overlap_kernel,
        out_shape=(
            jax.ShapeDtypeStruct((64, 4, LANES), F32),
            jax.ShapeDtypeStruct((32, 64, LANES), BF16),
        ),
        name="overlap",
        compiler_params=LIMIT,
    )(applied, *phis)


def project_kernel(overlaps, slab, *refs):
    phis, out = refs[:8], refs[8]
    parts = jnp.concatenate(
        two_parts(jnp.concatenate([overlaps[:, n, :] for n in range(4)], axis=1)), axis=0
    )

    def step(n, carry):
        both = dot(parts, all_two_rows(phis, n))
        value = two_rows(slab, n).astype(F32) - (both[:64] + both[64:])
        out[2 * n] = value[:, :LANES]
        out[2 * n + 1] = value[:, LANES:]
        return carry

    lax.fori_loop(0, 16, step, 0, unroll=4)


def project(overlaps, slab, phis):
    return pl.pallas_call(
        project_kernel,
        out_shape=jax.ShapeDtypeStruct((32, 64, LANES), F32),
        name="project",
        compiler_params=LIMIT,
    )(overlaps, slab, *phis)


def settle_kernel(arrived, out):
    for y in range(4):
        for q in range(4):
            both = [arrived[2 * y + core, 64 * q : 64 * q + 64, :].reshape(8, 8, LANES) for core in range(2)]
            out[128 * y : 128 * y + 128, LANES * q : LANES * (q + 1)] = woven(*both).reshape(128, LANES)


def settle(arrived):
    return pl.pallas_call(
        settle_kernel,
        out_shape=jax.ShapeDtypeStruct((512, 512), F32),
        name="settle",
        compiler_params=LIMIT,
    )(arrived)


def shifted(value, axis, distance):
    size = lax.axis_size(axis)
    return lax.ppermute(value, axis, [(n, (n + distance) % size) for n in range(size)])


def gathered(slab):
    slabs = [slab]
    for distance in (1, 3, 2):
        slabs.append(shifted(slab, "band_0", distance))
    return slabs + [shifted(value, "band_2", 1) for value in slabs]


def total_of(value):
    owned = exchange(value, ACROSS).sum(axis=0)
    return exchange(jnp.broadcast_to(owned, value.shape), ACROSS)


def on_device(orbitals, partners):
    mine = compact(orbitals)
    others = []
    for slot in range(PARTNERS):
        others.append(partner(mine, BAND, slot))
    parts = tables()
    inverse = inverse_eigen()
    first = solve(mine, others[0], parts, inverse)
    first, others[1] = lax.optimization_barrier((first, others[1]))
    second = solve(mine, others[1], parts, inverse)
    applied = solve_last(partners, mine, others[2], parts, inverse, first, second)
    phi = exchange(spread(mine), ACROSS)
    phis = gathered(turned(phi))
    applied = exchange(applied, ACROSS)
    partial, slab = overlap(applied, phis)
    gradient = project(total_of(partial), slab, phis)
    return settle(exchange(gradient.reshape(8, 256, LANES), HELD))


def solution(mesh):
    torus = Mesh(
        mesh.devices.reshape(4, 16, 2, mesh.shape["pair"]), ("band_0", "band_1", "band_2", "pair")
    )
    in_specs = (P(BAND_PAIR, None), P(BAND_PAIR, None))
    out_specs = P(None, BAND_PAIR)
    return jax.shard_map(
        on_device, mesh=torus, in_specs=in_specs, out_specs=out_specs, check_vma=False
    )
```

```python
import math

import jax
import jax.numpy as jnp
import numpy as np
from jax import lax
from jax.experimental import pallas as pl
from jax.experimental.pallas import tpu as pltpu
from jax.sharding import Mesh
from jax.sharding import PartitionSpec as P


NG = 64
PARTNERS = 3
NG3 = 262144
LANES = 128
ROWS = NG3 // LANES
BAND = ("band_0", "band_1", "band_2")
BAND_PAIR = ("band_0", "band_1", "band_2", "pair")
ACROSS = ("band_1", "pair")
HELD = ("band_0", "band_2")
F32, BF16 = jnp.float32, jnp.bfloat16
LIMIT = pltpu.CompilerParams(vmem_limit_bytes=16 * 2**20)


screening = 0.05


def partner(value, axis, distance):
    mask = 2**distance
    pairs = [(source, source ^ mask) for source in range(lax.axis_size(axis))]
    return lax.ppermute(value, axis, pairs)


def two_parts(value):
    high = value.astype(BF16)
    return high, (value - high.astype(F32)).astype(BF16)


def tables():
    steps = np.arange(NG) + 1
    table = np.sqrt(2.0 / (NG + 1)) * np.sin(np.pi * (np.outer(steps, steps) % (2 * NG + 2)) / (NG + 1))
    order = np.concatenate([np.arange(0, NG, 2), np.arange(1, NG, 2)])
    high = table.astype(BF16).astype(np.float64)
    low = table - high
    z_high, z_low = (np.kron(np.eye(2), part) for part in (high, low))
    high_y, low_y = (part[order][:, order] for part in (high, low))
    parts = (
        np.concatenate([z_high, z_high], axis=0),
        z_low,
        np.concatenate([high_y, high_y, low_y], axis=1),
        np.concatenate([high, high, low], axis=1),
    )
    return [jnp.asarray(part.astype(BF16)) for part in parts]


def compact_kernel(raw, out):
    def step(n, carry):
        rows = pl.ds(pl.multiple_of(n * 128, 128), 128)
        out[rows] = raw[rows, 0, :]
        return carry

    lax.fori_loop(0, ROWS // 128, step, 0)


def compact(raw):
    return pl.pallas_call(
        compact_kernel, out_shape=jax.ShapeDtypeStruct((ROWS, LANES), BF16), name="compact",
        compiler_params=LIMIT
    )(raw.reshape(ROWS, 1, LANES))


def inverse_kernel(out):
    def lam(index):
        return 2.0 - 2.0 * jnp.cos(math.pi * (index.astype(F32) + 1.0) / (NG + 1))

    shape = (NG, LANES)
    lane = lax.broadcasted_iota(jnp.int32, shape, 1)
    base = lam(lax.broadcasted_iota(jnp.int32, shape, 0)) + lam(lane % NG) + screening

    def step(pair, carry):
        y = lax.broadcasted_iota(jnp.int32, (8, LANES), 1) // NG + 2 * pair
        out[pair] = 1.0 / (base + jnp.broadcast_to(lam(y)[0:1], shape))
        return carry

    lax.fori_loop(0, NG // 2, step, 0)


def inverse_eigen():
    return pl.pallas_call(
        inverse_kernel, out_shape=jax.ShapeDtypeStruct((NG // 2, NG, LANES), F32), name="inverse",
        compiler_params=LIMIT
    )()


def dot(a, b):
    return jnp.dot(a, b, preferred_element_type=F32)


def side(table, value):
    high, low = two_parts(value)
    return dot(table, jnp.concatenate([high, low, high], axis=0))


def along_z(value, z_main, z_low):
    high, low = two_parts(value)
    return dot(jnp.concatenate([high, low], axis=1), z_main) + dot(high, z_low)


def swap_halves(rows, mask):
    first, second = rows[:32], rows[32:]
    top = jnp.where(mask, first, pltpu.roll(second, NG, 1))
    bottom = jnp.where(mask, pltpu.roll(first, NG, 1), second)
    return jnp.concatenate([top, bottom], axis=0)


def along_y(slabs, y_side, mask):
    moved = side(y_side, jnp.concatenate([swap_halves(s, mask) for s in slabs], axis=1))
    return [swap_halves(moved[:, LANES * n : LANES * (n + 1)], mask) for n in range(len(slabs))]


def pair_slabs(block, pair):
    start = 128 * pair
    return [block[start : start + 64], block[start + 64 : start + 128]]


def forward_part(own, other, z_main, z_low, y_side, field, mask):
    def step(n, carry):
        rows = pl.ds(pl.multiple_of(n * 256, 256), 256)
        density = own[rows].astype(F32) * other[rows].astype(F32)
        moved = along_z(density, z_main[...], z_low[...])
        for pair in range(2):
            for m, slab in enumerate(along_y(pair_slabs(moved, pair), y_side[...], mask)):
                field[pl.ds(n * 8 + 4 * pair + 2 * m, 2)] = slab.reshape(2, 32, LANES)
        return carry

    lax.fori_loop(0, ROWS // 256, step, 0, unroll=2)


def middle_part(x_side, inverse, field):
    def step(n, carry):
        group = pl.ds(pl.multiple_of(n * 8, 8), 8)
        block = jnp.transpose(field[:, group, :], (1, 0, 2))
        outs = []
        for pair in range(4):
            lines = [2 * pair, 2 * pair + 1]
            value = jnp.concatenate([block[m] for m in lines], axis=1)
            scale = jnp.concatenate([inverse[n * 8 + m] for m in lines], axis=1)
            value = side(x_side[...], side(x_side[...], value) * scale)
            outs += [value[:, :LANES], value[:, LANES:]]
        field[:, group, :] = jnp.transpose(jnp.stack(outs, axis=0), (1, 0, 2))
        return carry

    lax.fori_loop(0, 4, step, 0, unroll=2)


def backward_block(n, other, z_main, z_low, y_side, field, mask):
    rows = pl.ds(pl.multiple_of(n * 256, 256), 256)
    block = field[pl.ds(n * 8, 8)].reshape(256, LANES)
    slabs = []
    for pair in range(2):
        slabs += along_y(pair_slabs(block, pair), y_side[...], mask)
    moved = along_z(jnp.concatenate(slabs, axis=0), z_main[...], z_low[...])
    return rows, (moved * other[rows].astype(F32)).astype(BF16)


def solve_kernel(own, other, z_main, z_low, y_side, x_side, inverse, term, field):
    mask = lax.broadcasted_iota(jnp.int32, (32, LANES), 1) < NG
    forward_part(own, other, z_main, z_low, y_side, field, mask)
    middle_part(x_side, inverse, field)

    def step(n, carry):
        rows, value = backward_block(n, other, z_main, z_low, y_side, field, mask)
        term[rows] = value
        return carry

    lax.fori_loop(0, ROWS // 256, step, 0, unroll=2)


def woven(first, second):
    mask = lax.broadcasted_iota(jnp.int32, first.shape, 1) < 4
    top = jnp.where(mask, first, pltpu.roll(second, 4, 1))
    bottom = jnp.where(mask, pltpu.roll(first, 4, 1), second)
    return jnp.stack([top, bottom], axis=1).reshape(-1, 8, LANES)


def by_owner(rows):
    tiles = rows.reshape(8, 2, 2, 8, LANES)
    return woven(tiles[:, 0].reshape(16, 8, LANES), tiles[:, 1].reshape(16, 8, LANES))


def place(out, n, rows):
    start = pl.multiple_of(n // 2 * 8, 8)
    out[pl.ds(n % 2 * 32, 32), pl.ds(start, 8), :] = by_owner(rows).astype(BF16)


def spread_kernel(mine, out):
    def step(n, carry):
        place(out, n, mine[pl.ds(pl.multiple_of(n * 256, 256), 256)].astype(F32))
        return carry

    lax.fori_loop(0, ROWS // 256, step, 0, unroll=2)


def spread(mine):
    return pl.pallas_call(
        spread_kernel,
        out_shape=jax.ShapeDtypeStruct((64, 32, LANES), BF16),
        name="spread",
        compiler_params=LIMIT,
    )(mine)


def last_kernel(
    partners, own, other, z_main, z_low, y_side, x_side, inverse, first, second, out, field
):
    mask = lax.broadcasted_iota(jnp.int32, (32, LANES), 1) < NG
    forward_part(own, other, z_main, z_low, y_side, field, mask)
    middle_part(x_side, inverse, field)

    def step(n, carry):
        rows, third = backward_block(n, other, z_main, z_low, y_side, field, mask)
        total = jnp.zeros((256, LANES), F32)
        for slot, value in enumerate((first[rows], second[rows], third)):
            total = total + jnp.where(partners[0, slot] >= 0, value.astype(F32), 0.0)
        place(out, n, total)
        return carry

    lax.fori_loop(0, ROWS // 256, step, 0, unroll=2)


SLAB = pltpu.VMEM((32, 64, LANES), BF16)
FIELD = pltpu.VMEM((NG, NG // 2, LANES), F32)
VMEM = pl.BlockSpec(memory_space=pltpu.VMEM)
SMEM = pl.BlockSpec(memory_space=pltpu.SMEM)


def solve(own, other, parts, inverse):
    return pl.pallas_call(
        solve_kernel,
        out_shape=jax.ShapeDtypeStruct((ROWS, LANES), BF16),
        scratch_shapes=[FIELD],
        name="solve",
        compiler_params=LIMIT,
    )(own, other, *parts, inverse)


def solve_last(partners, own, other, parts, inverse, first, second):
    return pl.pallas_call(
        last_kernel,
        out_shape=jax.ShapeDtypeStruct((64, 32, LANES), BF16),
        in_specs=[SMEM] + [VMEM] * 9,
        scratch_shapes=[FIELD],
        name="last",
        compiler_params=LIMIT,
    )(partners, own, other, *parts, inverse, first, second)


def turn_to(value, out):
    for n in range(2):
        out[16 * n : 16 * n + 16] = jnp.transpose(value[:, 16 * n : 16 * n + 16, :], (1, 0, 2))


def turned(value):
    return pl.pallas_call(
        turn_to,
        out_shape=jax.ShapeDtypeStruct((32, 64, LANES), BF16),
        name="turn",
        compiler_params=LIMIT,
    )(value)


def exchange(value, axes):
    return lax.all_to_all(value, axes, split_axis=0, concat_axis=0, tiled=True)


def two_rows(slab, n):
    return jnp.concatenate([slab[2 * n], slab[2 * n + 1]], axis=1)


def all_two_rows(slabs, n):
    return jnp.concatenate([two_rows(slab, n) for slab in slabs], axis=0)


def overlap_kernel(applied, *refs):
    phis, (out, slab) = refs[:8], refs[8:]
    turn_to(applied, slab)

    def step(n, total):
        return total + lax.dot_general(
            two_rows(slab, n),
            all_two_rows(phis, n),
            (((1,), (1,)), ((), ())),
            preferred_element_type=F32,
        )

    total = lax.fori_loop(0, 16, step, jnp.zeros((64, 512), F32), unroll=4) * (1.0 / NG3)
    for n in range(4):
        out[:, n, :] = total[:, LANES * n : LANES * (n + 1)]


def overlap(applied, phis):
    return pl.pallas_call(
        overlap_kernel,
        out_shape=jax.ShapeDtypeStruct((64, 4, LANES), F32),
        scratch_shapes=[SLAB],
        name="overlap",
        compiler_params=LIMIT,
    )(applied, *phis)


def project_kernel(overlaps, applied, *refs):
    phis, (out, slab) = refs[:8], refs[8:]
    turn_to(applied, slab)
    parts = jnp.concatenate(
        two_parts(jnp.concatenate([overlaps[:, n, :] for n in range(4)], axis=1)), axis=0
    )

    def step(n, carry):
        both = dot(parts, all_two_rows(phis, n))
        value = two_rows(slab, n).astype(F32) - (both[:64] + both[64:])
        out[2 * n] = value[:, :LANES]
        out[2 * n + 1] = value[:, LANES:]
        return carry

    lax.fori_loop(0, 16, step, 0, unroll=4)


def project(overlaps, applied, phis):
    return pl.pallas_call(
        project_kernel,
        out_shape=jax.ShapeDtypeStruct((32, 64, LANES), F32),
        scratch_shapes=[SLAB],
        name="project",
        compiler_params=LIMIT,
    )(overlaps, applied, *phis)


def settle_kernel(arrived, out):
    for y in range(4):
        for q in range(4):
            both = [arrived[2 * y + core, 64 * q : 64 * q + 64, :].reshape(8, 8, LANES) for core in range(2)]
            out[128 * y : 128 * y + 128, LANES * q : LANES * (q + 1)] = woven(*both).reshape(128, LANES)


def settle(arrived):
    return pl.pallas_call(
        settle_kernel,
        out_shape=jax.ShapeDtypeStruct((512, 512), F32),
        name="settle",
        compiler_params=LIMIT,
    )(arrived)


def shifted(value, axis, distance):
    size = lax.axis_size(axis)
    return lax.ppermute(value, axis, [(n, (n + distance) % size) for n in range(size)])


def gathered(slab):
    slabs = [slab]
    for distance in (1, 3, 2):
        slabs.append(shifted(slab, "band_0", distance))
    return slabs + [shifted(value, "band_2", 1) for value in slabs]


def total_of(value):
    owned = exchange(value, ACROSS).sum(axis=0)
    return exchange(jnp.broadcast_to(owned, value.shape), ACROSS)


def on_device(orbitals, partners):
    mine = compact(orbitals)
    others = []
    for slot in range(PARTNERS):
        others.append(partner(mine, BAND, slot))
    parts = tables()
    inverse = inverse_eigen()
    first = solve(mine, others[0], parts, inverse)
    first, others[1] = lax.optimization_barrier((first, others[1]))
    second = solve(mine, others[1], parts, inverse)
    applied = solve_last(partners, mine, others[2], parts, inverse, first, second)
    phi = exchange(spread(mine), ACROSS)
    phis = gathered(turned(phi))
    applied = exchange(applied, ACROSS)
    gradient = project(total_of(overlap(applied, phis)), applied, phis)
    return settle(exchange(gradient.reshape(8, 256, LANES), HELD))


def solution(mesh):
    torus = Mesh(
        mesh.devices.reshape(4, 16, 2, mesh.shape["pair"]), ("band_0", "band_1", "band_2", "pair")
    )
    in_specs = (P(BAND_PAIR, None), P(BAND_PAIR, None))
    out_specs = P(None, BAND_PAIR)
    return jax.shard_map(
        on_device, mesh=torus, in_specs=in_specs, out_specs=out_specs, check_vma=False
    )
```

```python
import math

import jax
import jax.numpy as jnp
import numpy as np
from jax import lax
from jax.experimental import pallas as pl
from jax.experimental.pallas import tpu as pltpu
from jax.sharding import Mesh
from jax.sharding import PartitionSpec as P


NG = 64
PARTNERS = 3
NG3 = 262144
LANES = 128
ROWS = NG3 // LANES
BAND = ("band_0", "band_1", "band_2")
BAND_PAIR = ("band_0", "band_1", "band_2", "pair")
ACROSS = ("band_1", "pair")
HELD = ("band_0", "band_2")
F32, BF16 = jnp.float32, jnp.bfloat16
LIMIT = pltpu.CompilerParams(vmem_limit_bytes=16 * 2**20)


screening = 0.05


def partner(value, axis, distance):
    mask = 2**distance
    pairs = [(source, source ^ mask) for source in range(lax.axis_size(axis))]
    return lax.ppermute(value, axis, pairs)


def two_parts(value):
    high = value.astype(BF16)
    return high, (value - high.astype(F32)).astype(BF16)


def tables():
    steps = np.arange(NG) + 1
    table = np.sqrt(2.0 / (NG + 1)) * np.sin(np.pi * (np.outer(steps, steps) % (2 * NG + 2)) / (NG + 1))
    order = np.concatenate([np.arange(0, NG, 2), np.arange(1, NG, 2)])
    high = table.astype(BF16).astype(np.float64)
    low = table - high
    z_high, z_low = (np.kron(np.eye(2), part) for part in (high, low))
    high_y, low_y = (part[order][:, order] for part in (high, low))
    parts = (
        np.concatenate([z_high, z_high], axis=0),
        z_low,
        np.concatenate([high_y, high_y, low_y], axis=1),
        np.concatenate([high, high, low], axis=1),
    )
    return [jnp.asarray(part.astype(BF16)) for part in parts]


def compact_kernel(raw, out):
    def step(n, carry):
        rows = pl.ds(pl.multiple_of(n * 128, 128), 128)
        out[rows] = raw[rows, 0, :]
        return carry

    lax.fori_loop(0, ROWS // 128, step, 0)


def compact(raw):
    return pl.pallas_call(
        compact_kernel, out_shape=jax.ShapeDtypeStruct((ROWS, LANES), BF16), name="compact",
        compiler_params=LIMIT
    )(raw.reshape(ROWS, 1, LANES))


def inverse_kernel(out):
    def lam(index):
        return 2.0 - 2.0 * jnp.cos(math.pi * (index.astype(F32) + 1.0) / (NG + 1))

    shape = (NG, LANES)
    lane = lax.broadcasted_iota(jnp.int32, shape, 1)
    base = lam(lax.broadcasted_iota(jnp.int32, shape, 0)) + lam(lane % NG) + screening

    def step(pair, carry):
        y = lax.broadcasted_iota(jnp.int32, (8, LANES), 1) // NG + 2 * pair
        out[pair] = 1.0 / (base + jnp.broadcast_to(lam(y)[0:1], shape))
        return carry

    lax.fori_loop(0, NG // 2, step, 0)


def inverse_eigen():
    return pl.pallas_call(
        inverse_kernel, out_shape=jax.ShapeDtypeStruct((NG // 2, NG, LANES), F32), name="inverse",
        compiler_params=LIMIT
    )()


def dot(a, b):
    return jnp.dot(a, b, preferred_element_type=F32)


def side(table, value):
    high, low = two_parts(value)
    return dot(table, jnp.concatenate([high, low, high], axis=0))


def along_z(value, z_main, z_low):
    high, low = two_parts(value)
    return dot(jnp.concatenate([high, low], axis=1), z_main) + dot(high, z_low)


def swap_halves(rows, mask):
    first, second = rows[:32], rows[32:]
    top = jnp.where(mask, first, pltpu.roll(second, NG, 1))
    bottom = jnp.where(mask, pltpu.roll(first, NG, 1), second)
    return jnp.concatenate([top, bottom], axis=0)


def along_y(slabs, y_side, mask):
    moved = side(y_side, jnp.concatenate([swap_halves(s, mask) for s in slabs], axis=1))
    return [swap_halves(moved[:, LANES * n : LANES * (n + 1)], mask) for n in range(len(slabs))]


def pair_slabs(block, pair):
    start = 128 * pair
    return [block[start : start + 64], block[start + 64 : start + 128]]


def forward_part(own, other, z_main, z_low, y_side, field, mask):
    def step(n, carry):
        rows = pl.ds(pl.multiple_of(n * 256, 256), 256)
        density = own[rows].astype(F32) * other[rows].astype(F32)
        moved = along_z(density, z_main[...], z_low[...])
        for pair in range(2):
            for m, slab in enumerate(along_y(pair_slabs(moved, pair), y_side[...], mask)):
                field[pl.ds(n * 8 + 4 * pair + 2 * m, 2)] = slab.reshape(2, 32, LANES)
        return carry

    lax.fori_loop(0, ROWS // 256, step, 0, unroll=2)


def middle_part(x_side, inverse, field):
    def step(n, carry):
        group = pl.ds(pl.multiple_of(n * 8, 8), 8)
        block = jnp.transpose(field[:, group, :], (1, 0, 2))
        outs = []
        for pair in range(4):
            lines = [2 * pair, 2 * pair + 1]
            value = jnp.concatenate([block[m] for m in lines], axis=1)
            scale = jnp.concatenate([inverse[n * 8 + m] for m in lines], axis=1)
            value = side(x_side[...], side(x_side[...], value) * scale)
            outs += [value[:, :LANES], value[:, LANES:]]
        field[:, group, :] = jnp.transpose(jnp.stack(outs, axis=0), (1, 0, 2))
        return carry

    lax.fori_loop(0, 4, step, 0, unroll=2)


def backward_block(n, other, z_main, z_low, y_side, field, mask):
    rows = pl.ds(pl.multiple_of(n * 256, 256), 256)
    block = field[pl.ds(n * 8, 8)].reshape(256, LANES)
    slabs = []
    for pair in range(2):
        slabs += along_y(pair_slabs(block, pair), y_side[...], mask)
    moved = along_z(jnp.concatenate(slabs, axis=0), z_main[...], z_low[...])
    return rows, (moved * other[rows].astype(F32)).astype(BF16)


def solve_kernel(own, other, z_main, z_low, y_side, x_side, inverse, term, field):
    mask = lax.broadcasted_iota(jnp.int32, (32, LANES), 1) < NG
    forward_part(own, other, z_main, z_low, y_side, field, mask)
    middle_part(x_side, inverse, field)

    def step(n, carry):
        rows, value = backward_block(n, other, z_main, z_low, y_side, field, mask)
        term[rows] = value
        return carry

    lax.fori_loop(0, ROWS // 256, step, 0, unroll=2)


def woven(first, second):
    mask = lax.broadcasted_iota(jnp.int32, first.shape, 1) < 4
    top = jnp.where(mask, first, pltpu.roll(second, 4, 1))
    bottom = jnp.where(mask, pltpu.roll(first, 4, 1), second)
    return jnp.stack([top, bottom], axis=1).reshape(-1, 8, LANES)


def by_owner(rows):
    tiles = rows.reshape(8, 2, 2, 8, LANES)
    return woven(tiles[:, 0].reshape(16, 8, LANES), tiles[:, 1].reshape(16, 8, LANES))


def place(out, n, rows):
    start = pl.multiple_of(n // 2 * 8, 8)
    out[pl.ds(n % 2 * 32, 32), pl.ds(start, 8), :] = by_owner(rows).astype(BF16)


def spread_kernel(mine, out):
    def step(n, carry):
        place(out, n, mine[pl.ds(pl.multiple_of(n * 256, 256), 256)].astype(F32))
        return carry

    lax.fori_loop(0, ROWS // 256, step, 0, unroll=2)


def spread(mine):
    return pl.pallas_call(
        spread_kernel,
        out_shape=jax.ShapeDtypeStruct((64, 32, LANES), BF16),
        name="spread",
        compiler_params=LIMIT,
    )(mine)


def last_kernel(
    partners, own, other, z_main, z_low, y_side, x_side, inverse, first, second, out, field
):
    mask = lax.broadcasted_iota(jnp.int32, (32, LANES), 1) < NG
    forward_part(own, other, z_main, z_low, y_side, field, mask)
    middle_part(x_side, inverse, field)

    def step(n, carry):
        rows, third = backward_block(n, other, z_main, z_low, y_side, field, mask)
        total = jnp.zeros((256, LANES), F32)
        for slot, value in enumerate((first[rows], second[rows], third)):
            total = total + jnp.where(partners[0, slot] >= 0, value.astype(F32), 0.0)
        place(out, n, total)
        return carry

    lax.fori_loop(0, ROWS // 256, step, 0, unroll=2)


SLAB = pltpu.VMEM((32, 64, LANES), BF16)
FIELD = pltpu.VMEM((NG, NG // 2, LANES), F32)
VMEM = pl.BlockSpec(memory_space=pltpu.VMEM)
SMEM = pl.BlockSpec(memory_space=pltpu.SMEM)


def solve(own, other, parts, inverse):
    return pl.pallas_call(
        solve_kernel,
        out_shape=jax.ShapeDtypeStruct((ROWS, LANES), BF16),
        scratch_shapes=[FIELD],
        name="solve",
        compiler_params=LIMIT,
    )(own, other, *parts, inverse)


def solve_last(partners, own, other, parts, inverse, first, second):
    return pl.pallas_call(
        last_kernel,
        out_shape=jax.ShapeDtypeStruct((64, 32, LANES), BF16),
        in_specs=[SMEM] + [VMEM] * 9,
        scratch_shapes=[FIELD],
        name="last",
        compiler_params=LIMIT,
    )(partners, own, other, *parts, inverse, first, second)


def turn_to(value, out):
    for n in range(2):
        out[16 * n : 16 * n + 16] = jnp.transpose(value[:, 16 * n : 16 * n + 16, :], (1, 0, 2))


def turned(value):
    return pl.pallas_call(
        turn_to,
        out_shape=jax.ShapeDtypeStruct((32, 64, LANES), BF16),
        name="turn",
        compiler_params=LIMIT,
    )(value)


def exchange(value, axes):
    return lax.all_to_all(value, axes, split_axis=0, concat_axis=0, tiled=True)


def two_rows(slab, n):
    return jnp.concatenate([slab[2 * n], slab[2 * n + 1]], axis=1)


def all_two_rows(slabs, n):
    return jnp.concatenate([two_rows(slab, n) for slab in slabs], axis=0)


def overlap_kernel(applied, *refs):
    phis, before, (out, slab) = refs[:4], refs[4:-2], refs[-2:]
    turn_to(applied, slab)

    def step(n, total):
        return total + lax.dot_general(
            two_rows(slab, n),
            all_two_rows(phis, n),
            (((1,), (1,)), ((), ())),
            preferred_element_type=F32,
        )

    total = lax.fori_loop(0, 16, step, jnp.zeros((64, 256), F32), unroll=4) * (1.0 / NG3)
    for ref in before:
        out[:, 0:2, :] = ref[...]
    for n in range(2):
        out[:, 2 * len(before) + n, :] = total[:, LANES * n : LANES * (n + 1)]


def overlap(applied, phis, *before):
    return pl.pallas_call(
        overlap_kernel,
        out_shape=jax.ShapeDtypeStruct((64, 2 + 2 * len(before), LANES), F32),
        scratch_shapes=[SLAB],
        name="overlap",
        compiler_params=LIMIT,
    )(applied, *phis, *before)


def project_kernel(overlaps, applied, *refs):
    phis, (out, slab) = refs[:8], refs[8:]
    turn_to(applied, slab)
    parts = jnp.concatenate(
        two_parts(jnp.concatenate([overlaps[:, n, :] for n in range(4)], axis=1)), axis=0
    )

    def step(n, carry):
        both = dot(parts, all_two_rows(phis, n))
        value = two_rows(slab, n).astype(F32) - (both[:64] + both[64:])
        out[2 * n] = value[:, :LANES]
        out[2 * n + 1] = value[:, LANES:]
        return carry

    lax.fori_loop(0, 16, step, 0, unroll=4)


def project(overlaps, applied, phis):
    return pl.pallas_call(
        project_kernel,
        out_shape=jax.ShapeDtypeStruct((32, 64, LANES), F32),
        scratch_shapes=[SLAB],
        name="project",
        compiler_params=LIMIT,
    )(overlaps, applied, *phis)


def settle_kernel(arrived, out):
    for y in range(4):
        for q in range(4):
            both = [arrived[2 * y + core, 64 * q : 64 * q + 64, :].reshape(8, 8, LANES) for core in range(2)]
            out[128 * y : 128 * y + 128, LANES * q : LANES * (q + 1)] = woven(*both).reshape(128, LANES)


def settle(arrived):
    return pl.pallas_call(
        settle_kernel,
        out_shape=jax.ShapeDtypeStruct((512, 512), F32),
        name="settle",
        compiler_params=LIMIT,
    )(arrived)


def shifted(value, axis, distance):
    size = lax.axis_size(axis)
    return lax.ppermute(value, axis, [(n, (n + distance) % size) for n in range(size)])


def gathered(slab):
    slabs = [slab]
    for distance in (2, 1, 3):
        slabs.append(shifted(slab, "band_0", distance))
    return slabs + [shifted(value, "band_2", 1) for value in slabs]


def total_of(value):
    owned = exchange(value, ACROSS).sum(axis=0)
    return exchange(jnp.broadcast_to(owned, value.shape), ACROSS)


def on_device(orbitals, partners):
    mine = compact(orbitals)
    others = []
    for slot in range(PARTNERS):
        others.append(partner(mine, BAND, slot))
    parts = tables()
    inverse = inverse_eigen()
    first = solve(mine, others[0], parts, inverse)
    first, others[1] = lax.optimization_barrier((first, others[1]))
    second = solve(mine, others[1], parts, inverse)
    applied = solve_last(partners, mine, others[2], parts, inverse, first, second)
    phi = exchange(spread(mine), ACROSS)
    phis = gathered(turned(phi))
    applied = exchange(applied, ACROSS)
    half = overlap(applied, phis[:4])
    gradient = project(total_of(overlap(applied, phis[4:], half)), applied, phis)
    return settle(exchange(gradient.reshape(8, 256, LANES), HELD))


def solution(mesh):
    torus = Mesh(
        mesh.devices.reshape(4, 16, 2, mesh.shape["pair"]), ("band_0", "band_1", "band_2", "pair")
    )
    in_specs = (P(BAND_PAIR, None), P(BAND_PAIR, None))
    out_specs = P(None, BAND_PAIR)
    return jax.shard_map(
        on_device, mesh=torus, in_specs=in_specs, out_specs=out_specs, check_vma=False
    )
```
